256 devices in a mesh: section: 8 (over x, core), fsdp: 32 (over y, z).
Axes of the slice: x: 4, y: 4, z: 8, core: 2. Of those that a mesh axis runs over, the one named last changes fastest.
Arguments:
- tokens: bfloat16 [8, 2, 4096, 8192], P('section', None, 'fsdp'), may hold values from -6 to 6
- queries: bfloat16 [8, 2, 4096, 4096], P('section', None, 'fsdp'), may hold values from -200 to 200
- gains: bfloat16 [8, 8192], P('section'), may hold values from 0.5 to 1.5
- key_weight: bfloat16 [8, 8192, 512], P('section', 'fsdp'), may hold values from -0.0625 to 0.0625
- value_weight: bfloat16 [8, 8192, 512], P('section', 'fsdp'), may hold values from -0.0625 to 0.0625
- lengths: int32 [2, 64], replicated, may hold values from 1 to 128, 4096 in all within a row
Outputs:
- attended: bfloat16 [8, 2, 4096, 4096], P('section', None, 'fsdp')
The draws below stay inside these ranges and needn't reach their ends.
Inputs may be any that keep to these rules, and one draw needn't show every extreme that they name: `lengths`: each row sums to 4096; some document has exactly 128 tokens.
All inputs are finite; a program needn't handle non-finite values.
Results may differ from the reference program's by a relative error of at most 0.012.
The reference program's roundings to bfloat16 on the way (of `normed`) count: a program that leaves them out, or rounds other values in their place, can miss the bound.
Values may be sent and summed in bfloat16 or wider, within the bound.
No kernel may reach another device: no remote copies, remote signals or barrier semaphores. Data moves between devices by JAX's collectives and lax.ppermute only.
A program may use at most 128 MiB of HBM per device.

```python
import math
import jax
import jax.numpy as jnp
import numpy as np
from jax import lax

D = 8192
KV_HEADS = 4
Q_HEADS = 32
HEAD = 128
MICRO = 2
TOK_DEV = 128
TOKENS = 4096
DOCS = 64
LAYERS = 8


def draw_queries(key, part):
    shape = (LAYERS, MICRO, TOKENS, Q_HEADS * HEAD)
    normal_part = jax.random.normal(jax.random.fold_in(key, 11), shape, jnp.float32)
    drawn = jnp.clip(normal_part, -6.0, 6.0)
    return drawn.astype(jnp.bfloat16)


def block_levels(stream_key, extent, pieces, low, high):
    def one(position, blocks):
        draws = jax.random.uniform(jax.random.fold_in(jax.random.fold_in(stream_key, 6), position), (blocks,), jnp.float32, low / len(pieces), high / len(pieces))
        return jnp.repeat(jnp.exp(draws), extent[position] // blocks).reshape((-1,) + (1,) * (len(extent) - position - 1))

    factor_of = one(*pieces[0])
    for cut in pieces[1:]:
        factor_of = factor_of * one(*cut)
    return factor_of


def profile(number_of, total, most, skew):
    portions = [(1 << 20) // math.isqrt(standing ** skew) + 1 for standing in range(2, number_of + 1)]
    spare, holding = total - most - (number_of - 1), [1] * (number_of - 1)
    while spare > 0:
        movable = [i for i in range(number_of - 1) if holding[i] < most]
        mass, remaining = sum([portions[i] for i in movable]), spare
        for i in movable:
            addition = min(most - holding[i], max(1, remaining * portions[i] // mass), spare)
            holding[i] = holding[i] + addition
            spare = spare - addition
    return np.array([most] + holding)


def ragged_sizes(rng, amount, total, most, slope):
    if amount == 2:
        one = jax.random.randint(rng, (), max(1, total - most), min(most, total - 1) + 1)
        return jnp.stack([one, total - one])
    sizes = jnp.asarray(profile(amount, total, most, slope), jnp.int32)
    couples = (amount - 1) // 2
    source_of, taker = sizes[1:1 + 2 * couples:2], sizes[2:2 + 2 * couples:2]
    room = jnp.minimum(source_of - 1, most - taker)
    passed = jax.random.randint(jax.random.fold_in(rng, 1), (couples,), 0, 1 << 20) % (room + 1)
    sizes = sizes.at[1:1 + 2 * couples:2].set(source_of - passed).at[2:2 + 2 * couples:2].set(taker + passed)
    return sizes[jax.random.permutation(jax.random.fold_in(rng, 2), amount)]


def scatter_about(own_key, dims, width, most, pieces=(), kind=jnp.bfloat16):
    values = jax.random.normal(own_key, dims, jnp.float32) * width
    if len(pieces) > 0:
        values = block_levels(own_key, dims, pieces, -0.22, 0.18) * values
    return jnp.clip(values, min=-most, max=most).astype(kind)


def setup_inputs(seed: int = 0) -> dict:
    key_list = jax.random.split(jax.random.key(seed), 7)
    return {
        "tokens": scatter_about(key_list[0], (LAYERS, MICRO, TOKENS, D), 1.0, 6.0, ((0, 8), (2, 32))),
        "queries": draw_queries(jax.random.fold_in(key_list[6], 71), 0),
        "gains": jnp.clip(1.0 + 0.1 * jax.random.normal(key_list[2], (LAYERS, D), jnp.float32), 0.5, 1.5).astype(jnp.bfloat16),
        "key_weight": scatter_about(key_list[3], (LAYERS, D, KV_HEADS * HEAD), D ** -0.5, 0.0625, ((0, 8), (1, 32))),
        "value_weight": scatter_about(key_list[4], (LAYERS, D, KV_HEADS * HEAD), D ** -0.5, 0.0625, ((0, 8), (1, 32))),
        "lengths": jax.vmap(lambda own: ragged_sizes(own, DOCS, TOKENS, TOK_DEV, 2))(jax.random.split(key_list[5], MICRO)).reshape((MICRO, DOCS)).astype(jnp.int32),
    }


def rms_norm(hidden, gain_row):
    widened = hidden.astype(jnp.float32)
    inverse_rms = lax.rsqrt(lax.optimization_barrier(jnp.mean(widened * widened, axis=-1, keepdims=True)) + 1e-05)
    return (widened * inverse_rms * gain_row.astype(jnp.float32)).astype(jnp.bfloat16)

def document_ids(length_row, positions):
    bounds = jnp.cumsum(length_row.astype(jnp.int32))
    return lax.optimization_barrier(jnp.sum((bounds[None, :] <= positions[:, None]).astype(jnp.int32), axis=1))

def block_attend(query_rows, key_rows, value_rows, query_pos, key_pos, query_doc, key_doc):
    query_count = query_rows.shape[0]
    key_count = key_rows.shape[0]
    kv_count = key_rows.shape[1] // HEAD
    group_count = query_rows.shape[1] // (kv_count * HEAD)
    query_heads = query_rows.reshape(query_count, kv_count, group_count, HEAD).astype(jnp.float32)
    key_heads = key_rows.reshape(key_count, kv_count, HEAD).astype(jnp.float32)
    value_heads = value_rows.reshape(key_count, kv_count, HEAD).astype(jnp.float32)
    scores = jnp.einsum('tkgd,skd->kgts', query_heads, key_heads) * HEAD ** (-0.5)
    allowed = (key_doc[None, :] == query_doc[:, None]) & (key_pos[None, :] <= query_pos[:, None]) & (key_pos[None, :] >= 0)
    scores = jnp.where(allowed, scores, -1e+30)
    maxima = lax.optimization_barrier(jnp.max(scores, axis=-1, keepdims=True))
    exponent = jnp.where(allowed, jnp.exp(scores - maxima), 0.0)
    totals = lax.optimization_barrier(jnp.sum(exponent, axis=-1, keepdims=True))
    softmax_rows = (exponent / totals).astype(jnp.bfloat16)
    mixed = jnp.einsum('kgts,skd->tkgd', softmax_rows.astype(jnp.float32), value_heads)
    return mixed.reshape(query_count, kv_count * group_count * HEAD).astype(jnp.bfloat16)

def attend_all(query_all, key_all, value_all, length_row):
    block_count = TOKENS // TOK_DEV
    zero_rows = jnp.zeros((TOK_DEV, key_all.shape[1]), jnp.bfloat16)
    padded_keys = jnp.concatenate([zero_rows, key_all], axis=0)
    padded_values = jnp.concatenate([zero_rows, value_all], axis=0)

    def attend_block(block_index):
        block_start = (block_index * TOK_DEV).astype(jnp.int32)
        query_rows = lax.dynamic_slice_in_dim(query_all, block_start, TOK_DEV, 0)
        key_rows = lax.dynamic_slice_in_dim(padded_keys, block_start, 2 * TOK_DEV, 0)
        value_rows = lax.dynamic_slice_in_dim(padded_values, block_start, 2 * TOK_DEV, 0)
        query_pos = block_start + jnp.arange(TOK_DEV, dtype=jnp.int32)
        key_pos = block_start - TOK_DEV + jnp.arange(2 * TOK_DEV, dtype=jnp.int32)
        return block_attend(query_rows, key_rows, value_rows, query_pos, key_pos, document_ids(length_row, query_pos), document_ids(length_row, key_pos))
    blocks_out = lax.map(attend_block, jnp.arange(block_count, dtype=jnp.int32))
    return blocks_out.reshape(TOKENS, query_all.shape[1])

def reference(tokens, queries, gains, key_weight, value_weight, lengths):
    results = []
    for slot_index in range(MICRO):
        per_layer = []
        for layer_index in range(LAYERS):
            normed = rms_norm(tokens[layer_index, slot_index], gains[layer_index])
            key_all = jnp.dot(normed, key_weight[layer_index], preferred_element_type=jnp.float32).astype(jnp.bfloat16)
            value_all = jnp.dot(normed, value_weight[layer_index], preferred_element_type=jnp.float32).astype(jnp.bfloat16)
            per_layer.append(attend_all(queries[layer_index, slot_index], key_all, value_all, lengths[slot_index]))
        results.append(jnp.stack(per_layer))
    return jnp.stack(results, axis=1)
```

```python
import jax
import jax.numpy as jnp
from jax import lax
from jax.experimental import pallas as pl
from jax.experimental.pallas import tpu as pltpu
from jax.sharding import Mesh, PartitionSpec as P


HEAD = 128
Y, Z = 4, 8


def cost(flops, nbytes):
    return pl.CostEstimate(flops=flops, bytes_accessed=nbytes, transcendentals=0)


def vmem():
    return pl.BlockSpec(memory_space=pltpu.VMEM)


def any_space():
    return pl.BlockSpec(memory_space=pl.ANY)


def norm_kernel(y_ref, x_ref, g_ref, *out_refs):
    x = x_ref[...].astype(jnp.float32)
    inv = lax.rsqrt(jnp.mean(x * x, axis=-1, keepdims=True) + 1e-05)
    width = x_ref.shape[1] // Y
    for j in range(Y):
        at = pl.multiple_of(((y_ref[0] + j) % Y) * width, width)
        cols = x_ref[:, pl.ds(at, width)].astype(jnp.float32)
        gain = g_ref[:, pl.ds(at, width)].astype(jnp.float32)
        out_refs[j][...] = (cols * inv * gain).astype(jnp.bfloat16)


def norm_quarters(rows, gain, y_index):
    count, width = rows.shape
    step = 32
    return pl.pallas_call(
        norm_kernel,
        grid_spec=pltpu.PrefetchScalarGridSpec(
            num_scalar_prefetch=1,
            grid=(count // step,),
            in_specs=[
                pl.BlockSpec((step, width), lambda i, y: (i, 0)),
                pl.BlockSpec((1, width), lambda i, y: (0, 0)),
            ],
            out_specs=[pl.BlockSpec((step, width // Y), lambda i, y: (i, 0))] * Y,
        ),
        out_shape=[jax.ShapeDtypeStruct((count, width // Y), jnp.bfloat16)] * Y,
        cost_estimate=cost(20_000_000, 8 << 20),
        name="norm",
    )(y_index, rows, gain)


def product_kernel(slot_ref, *refs):
    a_refs, w_refs, refs = refs[:Y], refs[Y : Y + Z], refs[Y + Z :]
    own_refs, send_refs = refs[:2], refs[2:8]
    a_buf, wk, wv, a_sem, w_sem = refs[8:]
    deep = wk.shape[0] // Z
    copies = []
    for j in range(Z):
        at = pl.multiple_of(slot_ref[j] * deep, deep)
        for h, buf in enumerate((wk, wv)):
            c = pltpu.make_async_copy(w_refs[j].at[h], buf.at[pl.ds(at, deep)], w_sem.at[2 * j + h])
            c.start()
            copies.append(c)
    loads = [pltpu.make_async_copy(a_refs[j], a_buf.at[j], a_sem.at[j]) for j in range(Y)]
    for c in loads:
        c.start()
    for c in copies:
        c.wait()
    wide = wk.shape[1]
    half = a_buf.shape[1] // 2
    for j in range(Y):
        loads[j].wait()
        k = jnp.dot(a_buf[j], wk[...], preferred_element_type=jnp.float32)
        v = jnp.dot(a_buf[j], wv[...], preferred_element_type=jnp.float32)
        for m in range(2):
            km, vm = k[m * half : (m + 1) * half], v[m * half : (m + 1) * half]
            if j == 0:
                own_refs[m][:, :wide] = km
                own_refs[m][:, wide:] = vm
            else:
                high = km.astype(jnp.bfloat16)
                out = send_refs[3 * m + j - 1]
                out[:, :wide] = high
                out[:, wide : 2 * wide] = (km - high.astype(jnp.float32)).astype(jnp.bfloat16)
                out[:, 2 * wide :] = vm.astype(jnp.bfloat16)


def products(slots, acts, weights):
    rows, deep = acts[0].shape
    wide = weights[0].shape[2]
    half = rows // 2
    own = jax.ShapeDtypeStruct((half, 2 * wide), jnp.float32)
    send = jax.ShapeDtypeStruct((half, 3 * wide), jnp.bfloat16)
    return pl.pallas_call(
        product_kernel,
        in_specs=[pl.BlockSpec(memory_space=pltpu.SMEM)] + [any_space()] * (Y + Z),
        out_specs=[vmem()] * 8,
        out_shape=[own] * 2 + [send] * 6,
        scratch_shapes=[
            pltpu.VMEM((Y, rows, deep), jnp.bfloat16),
            pltpu.VMEM((deep, wide), jnp.bfloat16),
            pltpu.VMEM((deep, wide), jnp.bfloat16),
            pltpu.SemaphoreType.DMA((Y,)),
            pltpu.SemaphoreType.DMA((2 * Z,)),
        ],
        cost_estimate=cost(4 * Y * rows * deep * wide, 12 << 20),
        compiler_params=pltpu.CompilerParams(vmem_limit_bytes=40 << 20),
        name="products",
    )(slots, *acts, *weights)


def total_kernel(own_ref, *refs):
    parts, out_ref = refs[:3], refs[3]
    wide = own_ref.shape[1] // 2
    k, v = own_ref[:, :wide], own_ref[:, wide:]
    for p in parts:
        k = k + (p[:, :wide].astype(jnp.float32) + p[:, wide : 2 * wide].astype(jnp.float32))
        v = v + p[:, 2 * wide :].astype(jnp.float32)
    out_ref[:, :wide] = k.astype(jnp.bfloat16)
    out_ref[:, wide:] = v.astype(jnp.bfloat16)


def totals(own, parts):
    return pl.pallas_call(
        total_kernel,
        in_specs=[vmem()] * 4,
        out_specs=vmem(),
        out_shape=jax.ShapeDtypeStruct(own.shape, jnp.bfloat16),
        cost_estimate=cost(2_000_000, 2 << 20),
        name="totals",
    )(own, *parts)


def attend_kernel(first_ref, q_ref, pk_ref, k_ref, pv_ref, v_ref, *rest):
    out_ref = rest[-1]
    count = q_ref.shape[1]
    keys = jnp.concatenate([pk_ref[...], k_ref[...]], axis=0)
    values = jnp.concatenate([pv_ref[...], v_ref[...]], axis=0)
    column = lax.broadcasted_iota(jnp.int32, (count, 2 * count), 1)
    row = lax.broadcasted_iota(jnp.int32, (count, 2 * count), 0)
    allowed = (column >= first_ref[...]) & (column <= row + count)
    for g in range(q_ref.shape[2] // HEAD):
        q = q_ref[0, :, g * HEAD : (g + 1) * HEAD]
        s = lax.dot_general(q, keys, (((1,), (1,)), ((), ())), preferred_element_type=jnp.float32)
        s = jnp.where(allowed, s * HEAD ** (-0.5), -1e30)
        e = jnp.exp(s - jnp.max(s, axis=-1, keepdims=True))
        total = jnp.sum(e, axis=-1, keepdims=True)
        o = jnp.dot(e.astype(jnp.bfloat16), values, preferred_element_type=jnp.float32)
        out_ref[0, :, g * HEAD : (g + 1) * HEAD] = (o / total).astype(jnp.bfloat16)


def attend(slot, first, queries, prior, own, so_far):
    count, width = queries.shape[1], queries.shape[2]
    heads = own.shape[1] // (2 * HEAD)
    group = width // heads
    q_spec = pl.BlockSpec((1, count, group), lambda h: (slot, 0, h))
    k_spec = pl.BlockSpec((count, HEAD), lambda h: (0, h))
    v_spec = pl.BlockSpec((count, HEAD), lambda h: (0, h + heads))
    extra = [] if so_far is None else [so_far]
    return pl.pallas_call(
        attend_kernel,
        grid=(heads,),
        in_specs=[pl.BlockSpec((count, 1), lambda h: (0, 0)), q_spec, k_spec, k_spec, v_spec, v_spec]
        + [any_space()] * len(extra),
        out_specs=q_spec,
        out_shape=jax.ShapeDtypeStruct(queries.shape, jnp.bfloat16),
        input_output_aliases={6: 0} if extra else {},
        cost_estimate=cost(8 * count * count * width, 4 << 20),
        name="attend",
    )(first, queries, prior, own, prior, own, *extra)


def hop(block, axis, count, distance):
    return lax.ppermute(block, axis, [(i, (i + distance) % count) for i in range(count)])


def body(tokens, queries, gains, key_weight, value_weight, lengths):
    slots, count, width = tokens.shape[1:]
    y, z = lax.axis_index("y"), lax.axis_index("z")

    own_w = jnp.concatenate([key_weight, value_weight], axis=0)
    shards = [own_w]
    up = down = own_w
    ups, downs = [], []
    for _ in range(Z // 2 - 1):
        up = hop(up, "z", Z, 1)
        down = hop(down, "z", Z, -1)
        ups.append(up)
        downs.append(down)
    far_k = hop(up[:1], "z", Z, 1)
    far_v = hop(down[1:], "z", Z, -1)
    far = jnp.concatenate([far_k, far_v], axis=0)
    shards = [own_w] + ups + downs + [far]
    offsets = [0] + [s + 1 for s in range(Z // 2 - 1)] + [-s - 1 for s in range(Z // 2 - 1)] + [Z // 2]
    places = (z - jnp.array(offsets, jnp.int32)) % Z

    quarters = norm_quarters(
        tokens[0].reshape(slots * count, width), gains, y.reshape(1).astype(jnp.int32)
    )
    acts = [quarters[0]]
    for j in range(1, Y):
        acts.append(hop(quarters[j], "y", Y, j))

    pieces = products(places, acts, shards)
    own_parts, sends = pieces[:2], pieces[2:]

    bounds = jnp.sum(
        jnp.where(
            jnp.arange(lengths.shape[1])[None, :, None] <= jnp.arange(lengths.shape[1])[None, None, :],
            lengths[:, :, None],
            0,
        ),
        axis=1,
    )
    base = (y * Z + z) * count
    position = base + jnp.arange(count, dtype=jnp.int32)
    first = jnp.max(
        jnp.where(bounds[:, None, :] <= position[None, :, None], bounds[:, None, :], 0),
        axis=2,
        keepdims=True,
    )
    first = first - (base - count)

    back = []
    for m in range(slots):
        got = []
        for j in range(1, Y):
            got.append(hop(sends[3 * m + j - 1], "y", Y, -j))
        back.append(got)
    out = None
    for m in range(slots):
        own = totals(own_parts[m], back[m])
        prior = hop(own, ("y", "z"), Y * Z, 1)
        out = attend(m, first[m], queries[0], prior, own, out)
    return out[None]


def solution(mesh):
    split = Mesh(mesh.devices.reshape(-1, Y, Z), ("section", "y", "z"))
    spread = ("y", "z")

    return jax.shard_map(
        body,
        mesh=split,
        in_specs=(
            P("section", None, spread, None),
            P("section", None, spread, None),
            P("section", None),
            P("section", spread, None),
            P("section", spread, None),
            P(),
        ),
        out_specs=P("section", None, spread, None),
        check_vma=False,
    )
```

```python
import functools

import jax
import jax.numpy as jnp
from jax import lax
from jax.experimental import pallas as pl
from jax.experimental.pallas import tpu as pltpu
from jax.sharding import Mesh, PartitionSpec as P


HEAD = 128
Y, Z = 4, 8
VMEM = 67_043_328


def cost(flops, nbytes):
    return pl.CostEstimate(flops=flops, bytes_accessed=nbytes, transcendentals=0)


def vmem():
    return pl.BlockSpec(memory_space=pltpu.VMEM)


def hbm():
    return pl.BlockSpec(memory_space=pltpu.HBM)


def any_space():
    return pl.BlockSpec(memory_space=pl.ANY)


def pair_kernel(k_ref, v_ref, out_ref, sem):
    loads = [pltpu.make_async_copy(r.at[0], out_ref.at[i], sem.at[i]) for i, r in enumerate((k_ref, v_ref))]
    for c in loads:
        c.start()
    for c in loads:
        c.wait()


def pair(key_weight, value_weight):
    return pl.pallas_call(
        pair_kernel,
        in_specs=[hbm()] * 2,
        out_specs=vmem(),
        out_shape=jax.ShapeDtypeStruct((2,) + key_weight.shape[1:], key_weight.dtype),
        scratch_shapes=[pltpu.SemaphoreType.DMA((2,))],
        cost_estimate=cost(1_000_000, 1 << 20),
        compiler_params=pltpu.CompilerParams(vmem_limit_bytes=VMEM - (720 << 10)),
        name="pair",
    )(key_weight, value_weight)


CAME = [0] + [s + 1 for s in range(Z // 2 - 1)] + [-s - 1 for s in range(Z // 2 - 1)] + [Z // 2]
CHUNKS = 4


def norm_kernel(m, x_ref, g_ref, *refs):
    out_refs, x_buf, sem = refs[:Y], refs[Y], refs[Y + 1]
    y, z = lax.axis_index("y"), lax.axis_index("z")
    count = x_ref.shape[1] // CHUNKS
    loads = [pltpu.make_async_copy(x_ref.at[m, pl.ds(c * count, count)], x_buf.at[c], sem.at[c]) for c in range(CHUNKS)]
    for load in loads:
        load.start()
    wide = x_ref.shape[2] // (Y * Z)
    for c in range(CHUNKS):
        loads[c].wait()
        x = x_buf[c].astype(jnp.float32)
        inv = lax.rsqrt(jnp.mean(x * x, axis=-1, keepdims=True) + 1e-05)
        rows = slice(c * count, (c + 1) * count)
        for j in range(Y):
            for i in range(Z):
                at = ((y + j) & (Y - 1)) * Z + ((z - CAME[i]) & (Z - 1))
                at = pl.multiple_of(at * wide, wide)
                cols = x_buf[c, :, pl.ds(at, wide)].astype(jnp.float32)
                gain = g_ref[:, pl.ds(at, wide)].astype(jnp.float32)
                out_refs[j][rows, i * wide : (i + 1) * wide] = (cols * inv * gain).astype(jnp.bfloat16)


def norm_quarters(m, tokens, gain):
    _, count, width = tokens.shape
    return pl.pallas_call(
        functools.partial(norm_kernel, m),
        in_specs=[hbm(), vmem()],
        out_specs=[vmem()] * Y,
        out_shape=[jax.ShapeDtypeStruct((count, width // Y), jnp.bfloat16)] * Y,
        scratch_shapes=[
            pltpu.VMEM((CHUNKS, count // CHUNKS, width), jnp.bfloat16),
            pltpu.SemaphoreType.DMA((CHUNKS,)),
        ],
        cost_estimate=cost(10_000_000, 4 << 20),
        compiler_params=pltpu.CompilerParams(vmem_limit_bytes=VMEM - ((6656, 10240)[m] << 10)),
        name="norm",
    )(tokens, gain)


def product_kernel(*refs):
    a_refs, w_refs, far_refs = refs[:Y], refs[Y : Y + Z - 1], refs[Y + Z - 1 : Y + Z + 1]
    own_ref, send_refs = refs[Y + Z + 1], refs[Y + Z + 2 :]
    count, wide = a_refs[0].shape[0], w_refs[0].shape[2]
    a = jnp.concatenate([r[...] for r in a_refs], axis=0)
    wk = jnp.concatenate([r[0] for r in w_refs] + [far_refs[0][0]], axis=0)
    wv = jnp.concatenate([r[1] for r in w_refs] + [far_refs[1][0]], axis=0)
    k = jnp.dot(a, wk, preferred_element_type=jnp.float32)
    v = jnp.dot(a, wv, preferred_element_type=jnp.float32)
    own_ref[:, :wide] = k[:count]
    own_ref[:, wide:] = v[:count]
    for j in range(1, Y):
        kj, vj, out = k[j * count : (j + 1) * count], v[j * count : (j + 1) * count], send_refs[j - 1]
        high = kj.astype(jnp.bfloat16)
        out[:, :wide] = high
        out[:, wide : 2 * wide] = (kj - high.astype(jnp.float32)).astype(jnp.bfloat16)
        out[:, 2 * wide :] = vj.astype(jnp.bfloat16)


def products(acts, weights):
    rows, deep = acts[0].shape
    wide = weights[0].shape[2]
    return pl.pallas_call(
        product_kernel,
        in_specs=[vmem()] * (Y + Z + 1),
        out_specs=[vmem()] * Y,
        out_shape=[jax.ShapeDtypeStruct((rows, 2 * wide), jnp.float32)]
        + [jax.ShapeDtypeStruct((rows, 3 * wide), jnp.bfloat16)] * (Y - 1),
        cost_estimate=cost(4 * Y * rows * deep * wide, 8 << 20),
        compiler_params=pltpu.CompilerParams(vmem_limit_bytes=20 << 20),
        name="products",
    )(*acts, *weights)


def total_kernel(own_ref, *refs):
    parts, out_ref = refs[:3], refs[3]
    wide = own_ref.shape[1] // 2
    k, v = own_ref[:, :wide], own_ref[:, wide:]
    for p in parts:
        k = k + (p[:, :wide].astype(jnp.float32) + p[:, wide : 2 * wide].astype(jnp.float32))
        v = v + p[:, 2 * wide :].astype(jnp.float32)
    out_ref[:, :wide] = k.astype(jnp.bfloat16)
    out_ref[:, wide:] = v.astype(jnp.bfloat16)


def totals(own, parts):
    return pl.pallas_call(
        total_kernel,
        in_specs=[vmem()] * 4,
        out_specs=vmem(),
        out_shape=jax.ShapeDtypeStruct(own.shape, jnp.bfloat16),
        cost_estimate=cost(2_000_000, 2 << 20),
        compiler_params=pltpu.CompilerParams(vmem_limit_bytes=6 << 20),
        name="totals",
    )(own, *parts)


def attend_kernel(slot, len_ref, q_ref, pk_ref, k_ref, pv_ref, v_ref, *rest):
    out_ref = rest[-1]
    count, docs = q_ref.shape[1], len_ref.shape[1]
    before = lax.broadcasted_iota(jnp.int32, (docs, docs), 0) <= lax.broadcasted_iota(jnp.int32, (docs, docs), 1)
    lengths = len_ref[slot : slot + 1].astype(jnp.float32).astype(jnp.bfloat16)
    lengths = jnp.broadcast_to(lengths, (8, docs))
    ends = jnp.dot(lengths, before.astype(jnp.bfloat16), preferred_element_type=jnp.float32)[:1]
    ends = ends.astype(jnp.int32)
    base = (lax.axis_index("y") * Z + lax.axis_index("z")) * count
    position = base + lax.broadcasted_iota(jnp.int32, (count, docs), 0)
    first = jnp.max(jnp.where(ends <= position, ends, 0).astype(jnp.float32), axis=1, keepdims=True)
    first = first.astype(jnp.int32) - (base - count)
    column = lax.broadcasted_iota(jnp.int32, (count, 2 * count), 1)
    row = lax.broadcasted_iota(jnp.int32, (count, 2 * count), 0)
    allowed = (column >= first) & (column <= row + count)
    keys = jnp.concatenate([pk_ref[...], k_ref[...]], axis=0)
    values = jnp.concatenate([pv_ref[...], v_ref[...]], axis=0)
    values = jnp.concatenate([values, jnp.ones_like(values)], axis=1)
    for g in range(q_ref.shape[2] // HEAD):
        q = q_ref[0, :, g * HEAD : (g + 1) * HEAD]
        s = lax.dot_general(q, keys, (((1,), (1,)), ((), ())), preferred_element_type=jnp.float32)
        s = jnp.where(allowed, s * HEAD ** (-0.5), -1e30)
        e = jnp.exp(s - jnp.max(s, axis=-1, keepdims=True))
        o = jnp.dot(e.astype(jnp.bfloat16), values, preferred_element_type=jnp.float32)
        out_ref[0, :, g * HEAD : (g + 1) * HEAD] = (o[:, :HEAD] / o[:, HEAD:]).astype(jnp.bfloat16)


def attend(slot, lengths, queries, prior, own, so_far):
    count, width = queries.shape[1], queries.shape[2]
    heads = own.shape[1] // (2 * HEAD)
    group = width // heads
    q_spec = pl.BlockSpec((1, count, group), lambda h: (slot, 0, h))
    k_spec = pl.BlockSpec((count, HEAD), lambda h: (0, h))
    v_spec = pl.BlockSpec((count, HEAD), lambda h: (0, h + heads))
    extra = [] if so_far is None else [so_far]
    return pl.pallas_call(
        functools.partial(attend_kernel, slot),
        grid=(heads,),
        in_specs=[
            pl.BlockSpec(lengths.shape, lambda h: (0, 0)),
            q_spec,
            k_spec,
            k_spec,
            v_spec,
            v_spec,
        ]
        + [any_space()] * len(extra),
        out_specs=q_spec,
        out_shape=jax.ShapeDtypeStruct(queries.shape, jnp.bfloat16),
        input_output_aliases={6: 0} if extra else {},
        cost_estimate=cost(8 * count * count * width, 4 << 20),
        compiler_params=pltpu.CompilerParams(vmem_limit_bytes=10 << 20),
        name="attend",
    )(lengths, queries, prior, own, prior, own, *extra)


def hop(block, axis, count, distance, closed=True):
    return lax.ppermute(block, axis, [(i, (i + distance) % count) for i in range(count) if closed or i + distance < count])


def body(tokens, queries, gains, key_weight, value_weight, lengths):
    slots, _, _ = tokens.shape[1:]
    steps = Z // 2 - 1

    own_w = pair(key_weight, value_weight)
    up = down = own_w
    ups, downs = [], []
    for _ in range(steps):
        up = hop(up, "z", Z, 1)
        down = hop(down, "z", Z, -1)
        ups.append(up)
        downs.append(down)
    far_k = hop(up[:1], "z", Z, 1)
    far_v = hop(down[1:], "z", Z, -1)
    weights = [own_w] + ups + downs + [far_k, far_v]

    acts = []
    for m in range(slots):
        quarters = norm_quarters(m, tokens[0], gains)
        acts.append([quarters[0]] + [hop(quarters[j], "y", Y, j) for j in range(1, Y)])

    owns, parts = [], []
    for m in range(slots):
        own, *send = products(acts[m], weights)
        owns.append(own)
        parts.append([hop(send[j - 1], "y", Y, -j) for j in range(1, Y)])
    out = None
    for m in range(slots):
        own = totals(owns[m], parts[m])
        prior = hop(own, ("y", "z"), Y * Z, 1, closed=False)
        out = attend(m, lengths, queries[0], prior, own, out)
    return out[None]


def solution(mesh):
    split = Mesh(mesh.devices.reshape(-1, Y, Z), ("section", "y", "z"))
    spread = ("y", "z")

    return jax.shard_map(
        body,
        mesh=split,
        in_specs=(
            P("section", None, spread, None),
            P("section", None, spread, None),
            P("section", None),
            P("section", spread, None),
            P("section", spread, None),
            P(),
        ),
        out_specs=P("section", None, spread, None),
        check_vma=False,
    )
```

```python
import functools
import math

import jax
import jax.numpy as jnp
from jax import lax
from jax.experimental import pallas as pl
from jax.experimental.pallas import tpu as pltpu
from jax.sharding import Mesh, PartitionSpec as P


HEAD = 128
Y, Z = 4, 8


def cost(flops, nbytes):
    return pl.CostEstimate(flops=flops, bytes_accessed=nbytes, transcendentals=0)


def vmem():
    return pl.BlockSpec(memory_space=pltpu.VMEM)


def hbm():
    return pl.BlockSpec(memory_space=pltpu.HBM)


CAME = [0] + [s + 1 for s in range(Z // 2 - 1)] + [-s - 1 for s in range(Z // 2 - 1)] + [Z // 2]
CHUNKS = 4
NORM_GRANT = (51200, 46592)


def norm_kernel(m, x_ref, g_ref, *refs):
    out_refs, x_buf, sem = refs[:Y], refs[Y], refs[Y + 1]
    y, z = lax.axis_index("y"), lax.axis_index("z")
    count = x_ref.shape[1] // CHUNKS
    loads = [pltpu.make_async_copy(x_ref.at[m, pl.ds(c * count, count)], x_buf.at[c], sem.at[c]) for c in range(CHUNKS)]
    for load in loads:
        load.start()
    wide = x_ref.shape[2] // (Y * Z)
    for c in range(CHUNKS):
        loads[c].wait()
        x = x_buf[c].astype(jnp.float32)
        inv = lax.rsqrt(jnp.mean(x * x, axis=-1, keepdims=True) + 1e-05)
        rows = slice(c * count, (c + 1) * count)
        for j in range(Y):
            for i in range(Z):
                at = ((y + j) & (Y - 1)) * Z + ((z - CAME[i]) & (Z - 1))
                at = pl.multiple_of(at * wide, wide)
                cols = x_buf[c, :, pl.ds(at, wide)].astype(jnp.float32)
                gain = g_ref[:, pl.ds(at, wide)].astype(jnp.float32)
                out_refs[j][rows, i * wide : (i + 1) * wide] = (cols * inv * gain).astype(jnp.bfloat16)


def norm_quarters(m, tokens, gain):
    _, count, width = tokens.shape
    return pl.pallas_call(
        functools.partial(norm_kernel, m),
        in_specs=[hbm(), vmem()],
        out_specs=[vmem()] * Y,
        out_shape=[jax.ShapeDtypeStruct((count, width // Y), jnp.bfloat16)] * Y,
        scratch_shapes=[
            pltpu.VMEM((CHUNKS, count // CHUNKS, width), jnp.bfloat16),
            pltpu.SemaphoreType.DMA((CHUNKS,)),
        ],
        cost_estimate=cost(10_000_000, 4 << 20),
        compiler_params=pltpu.CompilerParams(vmem_limit_bytes=NORM_GRANT[m] << 10),
        name="norm",
    )(tokens, gain)


def packed(ref, rows, k, v):
    wide = k.shape[1]
    high = k.astype(jnp.bfloat16)
    ref[rows, :wide] = high
    ref[rows, wide : 2 * wide] = (k - high.astype(jnp.float32)).astype(jnp.bfloat16)
    ref[rows, 2 * wide :] = v.astype(jnp.bfloat16)


def opened(ref, rows):
    wide = ref.shape[1] // 3
    k = ref[rows, :wide].astype(jnp.float32) + ref[rows, wide : 2 * wide].astype(jnp.float32)
    return k, ref[rows, 2 * wide :].astype(jnp.float32)


def product_kernel(*refs):
    a_refs, k_refs, v_refs = refs[:Y], refs[Y : Y + Z], refs[Y + Z : Y + 2 * Z]
    own_ref, keep_ref, up_ref, down_ref = refs[Y + 2 * Z :]
    count, wide = a_refs[0].shape[0], k_refs[0].shape[1]
    half = count // 2
    a = jnp.concatenate([r[...] for r in a_refs], axis=0)
    wk = jnp.concatenate([r[...] for r in k_refs], axis=0)
    wv = jnp.concatenate([r[...] for r in v_refs], axis=0)
    k = jnp.dot(a, wk, preferred_element_type=jnp.float32)
    v = jnp.dot(a, wv, preferred_element_type=jnp.float32)

    def part(j, h):
        rows = slice(j * count + h * half, j * count + (h + 1) * half)
        return k[rows], v[rows]

    top, bottom = slice(0, half), slice(half, count)
    own_ref[:, :wide], own_ref[:, wide:] = k[:count], v[:count]
    keep_ref[top, :wide], keep_ref[top, wide:] = part(3, 0)
    keep_ref[bottom, :wide], keep_ref[bottom, wide:] = part(1, 1)
    packed(up_ref, top, *part(2, 0))
    packed(up_ref, bottom, *part(3, 1))
    packed(down_ref, top, *part(1, 0))
    packed(down_ref, bottom, *part(2, 1))


def products(acts, key_rows, value_rows):
    rows, deep = acts[0].shape
    wide = key_rows[0].shape[1]
    return pl.pallas_call(
        product_kernel,
        in_specs=[vmem()] * (Y + 2 * Z),
        out_specs=[vmem()] * 4,
        out_shape=[jax.ShapeDtypeStruct((rows, 2 * wide), jnp.float32)] * 2
        + [jax.ShapeDtypeStruct((rows, 3 * wide), jnp.bfloat16)] * 2,
        cost_estimate=cost(4 * Y * rows * deep * wide, 8 << 20),
        compiler_params=pltpu.CompilerParams(vmem_limit_bytes=20 << 20),
        name="products",
    )(*acts, *key_rows, *value_rows)


def relay_kernel(keep_ref, up_ref, down_ref, on_up_ref, on_down_ref):
    half, wide = on_up_ref.shape[0], on_up_ref.shape[1] // 3
    for rows, came, on in ((slice(0, half), up_ref, on_up_ref), (slice(half, 2 * half), down_ref, on_down_ref)):
        k, v = opened(came, rows)
        packed(on, slice(0, half), k + keep_ref[rows, :wide], v + keep_ref[rows, wide:])


def relay(keep, up, down):
    half, width = up.shape[0] // 2, up.shape[1]
    return pl.pallas_call(
        relay_kernel,
        in_specs=[vmem()] * 3,
        out_specs=[vmem()] * 2,
        out_shape=[jax.ShapeDtypeStruct((half, width), jnp.bfloat16)] * 2,
        cost_estimate=cost(2_000_000, 2 << 20),
        compiler_params=pltpu.CompilerParams(vmem_limit_bytes=6 << 20),
        name="relay",
    )(keep, up, down)


def total_kernel(own_ref, up_ref, down_ref, on_up_ref, on_down_ref, out_ref):
    count, wide = own_ref.shape[0], own_ref.shape[1] // 2
    half = count // 2
    for rows, near, on in ((slice(0, half), down_ref, on_up_ref), (slice(half, count), up_ref, on_down_ref)):
        k, v = opened(near, rows)
        far_k, far_v = opened(on, slice(0, half))
        out_ref[rows, :wide] = (own_ref[rows, :wide] + k + far_k).astype(jnp.bfloat16)
        out_ref[rows, wide:] = (own_ref[rows, wide:] + v + far_v).astype(jnp.bfloat16)


def totals(own, up, down, on_up, on_down):
    return pl.pallas_call(
        total_kernel,
        in_specs=[vmem()] * 5,
        out_specs=vmem(),
        out_shape=jax.ShapeDtypeStruct(own.shape, jnp.bfloat16),
        cost_estimate=cost(2_000_000, 2 << 20),
        compiler_params=pltpu.CompilerParams(vmem_limit_bytes=6 << 20),
        name="totals",
    )(own, up, down, on_up, on_down)


def attend_kernel(slot, len_ref, q_ref, prior_ref, own_ref, *refs):
    out_ref, buf, sem = refs[-3:]
    count, width, docs = q_ref.shape[1], q_ref.shape[2], len_ref.shape[1]
    heads = own_ref.shape[1] // (2 * HEAD)
    group = width // heads
    before = lax.broadcasted_iota(jnp.int32, (docs, docs), 0) <= lax.broadcasted_iota(jnp.int32, (docs, docs), 1)
    lengths = len_ref[slot : slot + 1].astype(jnp.float32).astype(jnp.bfloat16)
    lengths = jnp.broadcast_to(lengths, (8, docs))
    ends = jnp.dot(lengths, before.astype(jnp.bfloat16), preferred_element_type=jnp.float32)[:1]
    ends = ends.astype(jnp.int32)
    base = (lax.axis_index("y") * Z + lax.axis_index("z")) * count
    position = base + lax.broadcasted_iota(jnp.int32, (count, docs), 0)
    first = jnp.max(jnp.where(ends <= position, ends, 0).astype(jnp.float32), axis=1, keepdims=True)
    first = first.astype(jnp.int32) - (base - count)
    column = lax.broadcasted_iota(jnp.int32, (count, 2 * count), 1)
    row = lax.broadcasted_iota(jnp.int32, (count, 2 * count), 0)
    allowed = (column >= first) & (column <= row + count)
    stores = []
    for h in range(heads):
        at, of = slice(h * HEAD, (h + 1) * HEAD), slice((heads + h) * HEAD, (heads + h + 1) * HEAD)
        keys = jnp.concatenate([prior_ref[:, at], own_ref[:, at]], axis=0)
        values = jnp.concatenate([prior_ref[:, of], own_ref[:, of]], axis=0)
        values = jnp.concatenate([values, jnp.ones_like(values)], axis=1)
        for g in range(group // HEAD):
            cols = slice(h * group + g * HEAD, h * group + (g + 1) * HEAD)
            s = lax.dot_general(
                q_ref[slot, :, cols], keys, (((1,), (1,)), ((), ())), preferred_element_type=jnp.float32
            )
            s = jnp.where(allowed, s, -1e30)
            e = jnp.exp2((s - jnp.max(s, axis=-1, keepdims=True)) * (HEAD**-0.5 * math.log2(math.e)))
            o = jnp.dot(e.astype(jnp.bfloat16), values, preferred_element_type=jnp.float32)
            buf[:, cols] = (o[:, :HEAD] / o[:, HEAD:]).astype(jnp.bfloat16)
        part = slice(h * group, (h + 1) * group)
        store = pltpu.make_async_copy(buf.at[:, part], out_ref.at[slot, :, part], sem.at[h])
        store.start()
        stores.append(store)
    for store in stores:
        store.wait()


def attend(slot, lengths, queries, prior, own, so_far):
    count, width = queries.shape[1], queries.shape[2]
    heads = own.shape[1] // (2 * HEAD)
    extra = [] if so_far is None else [so_far]
    return pl.pallas_call(
        functools.partial(attend_kernel, slot),
        in_specs=[vmem()] * 4 + [hbm()] * len(extra),
        out_specs=hbm(),
        out_shape=jax.ShapeDtypeStruct(queries.shape, jnp.bfloat16),
        scratch_shapes=[pltpu.VMEM((count, width), jnp.bfloat16), pltpu.SemaphoreType.DMA((heads,))],
        input_output_aliases={4: 0} if extra else {},
        cost_estimate=cost(8 * count * count * width, 4 << 20),
        compiler_params=pltpu.CompilerParams(vmem_limit_bytes=16 << 20),
        name="attend",
    )(lengths, queries, prior, own, *extra)


def hop(block, axis, count, distance, closed=True):
    return lax.ppermute(block, axis, [(i, (i + distance) % count) for i in range(count) if closed or i + distance < count])


def body(tokens, queries, gains, key_weight, value_weight, lengths):
    key_weight, value_weight = key_weight[0], value_weight[0]
    slots, _, _ = tokens.shape[1:]
    steps = Z // 2 - 1

    rows = {}
    for name, own in (("k", key_weight), ("v", value_weight)):
        rows[name, 0] = own
    for s in range(Z // 2):
        for name in "kv":
            if s < steps or name == "k":
                rows[name, s + 1] = hop(rows[name, s], "z", Z, 1)
            if s < steps or name == "v":
                rows[name, -s - 1] = hop(rows[name, -s], "z", Z, -1)
    rows["v", Z // 2] = rows["v", -(Z // 2)]
    key_rows, value_rows = ([rows[name, c] for c in CAME] for name in "kv")

    acts = []
    for m in range(slots):
        quarters = norm_quarters(m, tokens[0], gains)
        acts.append([quarters[0]] + [hop(quarters[j], "y", Y, j) for j in range(1, Y)])

    held = []
    for m in range(slots):
        own, keep, up, down = products(acts[m], key_rows, value_rows)
        up, down = hop(up, "y", Y, 1), hop(down, "y", Y, -1)
        held.append((own, keep, up, down))
    sums = []
    for m in range(slots):
        own, keep, up, down = held[m]
        on_up, on_down = relay(keep, up, down)
        on_up, on_down = hop(on_up, "y", Y, 1), hop(on_down, "y", Y, -1)
        sums.append(totals(own, up, down, on_up, on_down))
    out = None
    for m in range(slots):
        prior = hop(sums[m], ("y", "z"), Y * Z, 1, closed=False)
        out = attend(m, lengths, queries[0], prior, sums[m], out)
    return out[None]


def solution(mesh):
    split = Mesh(mesh.devices.reshape(-1, Y, Z), ("section", "y", "z"))
    spread = ("y", "z")

    return jax.shard_map(
        body,
        mesh=split,
        in_specs=(
            P("section", None, spread, None),
            P("section", None, spread, None),
            P("section", None),
            P("section", spread, None),
            P("section", spread, None),
            P(),
        ),
        out_specs=P("section", None, spread, None),
        check_vma=False,
    )
```

```python
import functools
import math

import jax
import jax.numpy as jnp
from jax import lax
from jax.experimental import pallas as pl
from jax.experimental.pallas import tpu as pltpu
from jax.sharding import Mesh, PartitionSpec as P


HEAD = 128
Y, Z = 4, 8


def cost(flops, nbytes):
    return pl.CostEstimate(flops=flops, bytes_accessed=nbytes, transcendentals=0)


def vmem():
    return pl.BlockSpec(memory_space=pltpu.VMEM)


def hbm():
    return pl.BlockSpec(memory_space=pltpu.HBM)


CAME = [0] + [s + 1 for s in range(Z // 2 - 1)] + [-s - 1 for s in range(Z // 2 - 1)] + [Z // 2]
CHUNKS = 4
NORM_GRANT = (51200, 46592)


def norm_kernel(m, x_ref, g_ref, *refs):
    out_refs, x_buf, sem = refs[:Y], refs[Y], refs[Y + 1]
    y, z = lax.axis_index("y"), lax.axis_index("z")
    count = x_ref.shape[1] // CHUNKS
    loads = [pltpu.make_async_copy(x_ref.at[m, pl.ds(c * count, count)], x_buf.at[c], sem.at[c]) for c in range(CHUNKS)]
    for load in loads:
        load.start()
    wide = x_ref.shape[2] // (Y * Z)
    for c in range(CHUNKS):
        loads[c].wait()
        x = x_buf[c].astype(jnp.float32)
        inv = lax.rsqrt(jnp.mean(x * x, axis=-1, keepdims=True) + 1e-05)
        rows = slice(c * count, (c + 1) * count)
        for j in range(Y):
            for i in range(Z):
                at = ((y + j) & (Y - 1)) * Z + ((z - CAME[i]) & (Z - 1))
                at = pl.multiple_of(at * wide, wide)
                cols = x_buf[c, :, pl.ds(at, wide)].astype(jnp.float32)
                gain = g_ref[:, pl.ds(at, wide)].astype(jnp.float32)
                out_refs[j][rows, i * wide : (i + 1) * wide] = (cols * inv * gain).astype(jnp.bfloat16)


def norm_quarters(m, tokens, gain):
    _, count, width = tokens.shape
    return pl.pallas_call(
        functools.partial(norm_kernel, m),
        in_specs=[hbm(), vmem()],
        out_specs=[vmem()] * Y,
        out_shape=[jax.ShapeDtypeStruct((count, width // Y), jnp.bfloat16)] * Y,
        scratch_shapes=[
            pltpu.VMEM((CHUNKS, count // CHUNKS, width), jnp.bfloat16),
            pltpu.SemaphoreType.DMA((CHUNKS,)),
        ],
        cost_estimate=cost(10_000_000, 4 << 20),
        compiler_params=pltpu.CompilerParams(vmem_limit_bytes=NORM_GRANT[m] << 10),
        name="norm",
    )(tokens, gain)


def packed(ref, rows, k, v):
    wide = k.shape[1]
    high = k.astype(jnp.bfloat16)
    ref[rows, :wide] = high
    ref[rows, wide : 2 * wide] = (k - high.astype(jnp.float32)).astype(jnp.bfloat16)
    ref[rows, 2 * wide :] = v.astype(jnp.bfloat16)


def opened(ref, rows):
    wide = ref.shape[1] // 3
    k = ref[rows, :wide].astype(jnp.float32) + ref[rows, wide : 2 * wide].astype(jnp.float32)
    return k, ref[rows, 2 * wide :].astype(jnp.float32)


def split_products(k, v, own_ref, keep_ref, up_ref, down_ref):
    count, wide = own_ref.shape[0], k.shape[1]
    half = count // 2

    def part(j, h):
        rows = slice(j * count + h * half, j * count + (h + 1) * half)
        return k[rows], v[rows]

    top, bottom = slice(0, half), slice(half, count)
    own_ref[:, :wide], own_ref[:, wide:] = k[:count], v[:count]
    keep_ref[top, :wide], keep_ref[top, wide:] = part(3, 0)
    keep_ref[bottom, :wide], keep_ref[bottom, wide:] = part(1, 1)
    packed(up_ref, top, *part(2, 0))
    packed(up_ref, bottom, *part(3, 1))
    packed(down_ref, top, *part(1, 0))
    packed(down_ref, bottom, *part(2, 1))


def product_kernel(a_refs, k_refs, v_refs, so_far, refs, first):
    cols = slice(first * k_refs[0].shape[0], (first + len(k_refs)) * k_refs[0].shape[0])
    a = jnp.concatenate([r[:, cols] for r in a_refs], axis=0)
    k = jnp.dot(a, jnp.concatenate([r[...] for r in k_refs], axis=0), preferred_element_type=jnp.float32)
    v = jnp.dot(a, jnp.concatenate([r[...] for r in v_refs], axis=0), preferred_element_type=jnp.float32)
    if so_far is not None:
        wide = k.shape[1]
        k, v = k + so_far[:, :wide], v + so_far[:, wide:]
    if len(refs) == 1:
        refs[0][:, : k.shape[1]], refs[0][:, k.shape[1] :] = k, v
    else:
        split_products(k, v, *refs)


def products(acts, key_rows, value_rows, first=0, so_far=None, last=True):
    rows, _ = acts[0].shape
    blocks, (block, wide) = len(key_rows), key_rows[0].shape
    extra = [] if so_far is None else [so_far]
    count = Y + 2 * blocks + len(extra)
    outs = [jax.ShapeDtypeStruct((Y * rows, 2 * wide), jnp.float32)]
    if last:
        outs = [jax.ShapeDtypeStruct((rows, 2 * wide), jnp.float32)] * 2
        outs += [jax.ShapeDtypeStruct((rows, 3 * wide), jnp.bfloat16)] * 2

    def kernel(*refs):
        ins, refs = refs[:count], refs[count:]
        a_refs, k_refs, v_refs = ins[:Y], ins[Y : Y + blocks], ins[Y + blocks : Y + 2 * blocks]
        product_kernel(a_refs, k_refs, v_refs, ins[-1] if extra else None, refs, first)

    return pl.pallas_call(
        kernel,
        in_specs=[vmem()] * count,
        out_specs=[vmem()] * len(outs),
        out_shape=outs,
        cost_estimate=cost(4 * Y * rows * blocks * block * wide, 8 << 20),
        compiler_params=pltpu.CompilerParams(vmem_limit_bytes=20 << 20),
        name="products",
    )(*acts, *key_rows, *value_rows, *extra)


def relay_kernel(keep_ref, up_ref, down_ref, on_up_ref, on_down_ref):
    half, wide = on_up_ref.shape[0], on_up_ref.shape[1] // 3
    for rows, came, on in ((slice(0, half), up_ref, on_up_ref), (slice(half, 2 * half), down_ref, on_down_ref)):
        k, v = opened(came, rows)
        packed(on, slice(0, half), k + keep_ref[rows, :wide], v + keep_ref[rows, wide:])


def relay(keep, up, down):
    half, width = up.shape[0] // 2, up.shape[1]
    return pl.pallas_call(
        relay_kernel,
        in_specs=[vmem()] * 3,
        out_specs=[vmem()] * 2,
        out_shape=[jax.ShapeDtypeStruct((half, width), jnp.bfloat16)] * 2,
        cost_estimate=cost(2_000_000, 2 << 20),
        compiler_params=pltpu.CompilerParams(vmem_limit_bytes=6 << 20),
        name="relay",
    )(keep, up, down)


def total_kernel(own_ref, up_ref, down_ref, on_up_ref, on_down_ref, out_ref):
    count, wide = own_ref.shape[0], own_ref.shape[1] // 2
    half = count // 2
    for rows, near, on in ((slice(0, half), down_ref, on_up_ref), (slice(half, count), up_ref, on_down_ref)):
        k, v = opened(near, rows)
        far_k, far_v = opened(on, slice(0, half))
        out_ref[rows, :wide] = (own_ref[rows, :wide] + k + far_k).astype(jnp.bfloat16)
        out_ref[rows, wide:] = (own_ref[rows, wide:] + v + far_v).astype(jnp.bfloat16)


def totals(own, up, down, on_up, on_down):
    return pl.pallas_call(
        total_kernel,
        in_specs=[vmem()] * 5,
        out_specs=vmem(),
        out_shape=jax.ShapeDtypeStruct(own.shape, jnp.bfloat16),
        cost_estimate=cost(2_000_000, 2 << 20),
        compiler_params=pltpu.CompilerParams(vmem_limit_bytes=6 << 20),
        name="totals",
    )(own, up, down, on_up, on_down)


def attend_kernel(slot, len_ref, q_ref, prior_ref, own_ref, *refs):
    out_ref, buf, sem = refs[-3:]
    count, width, docs = q_ref.shape[1], q_ref.shape[2], len_ref.shape[1]
    heads = own_ref.shape[1] // (2 * HEAD)
    group = width // heads
    before = lax.broadcasted_iota(jnp.int32, (docs, docs), 0) <= lax.broadcasted_iota(jnp.int32, (docs, docs), 1)
    lengths = len_ref[slot : slot + 1].astype(jnp.float32).astype(jnp.bfloat16)
    lengths = jnp.broadcast_to(lengths, (8, docs))
    ends = jnp.dot(lengths, before.astype(jnp.bfloat16), preferred_element_type=jnp.float32)[:1]
    ends = ends.astype(jnp.int32)
    base = (lax.axis_index("y") * Z + lax.axis_index("z")) * count
    position = base + lax.broadcasted_iota(jnp.int32, (count, docs), 0)
    first = jnp.max(jnp.where(ends <= position, ends, 0).astype(jnp.float32), axis=1, keepdims=True)
    first = first.astype(jnp.int32) - (base - count)
    column = lax.broadcasted_iota(jnp.int32, (count, 2 * count), 1)
    row = lax.broadcasted_iota(jnp.int32, (count, 2 * count), 0)
    allowed = (column >= first) & (column <= row + count)
    stores = []
    for h in range(heads):
        at, of = slice(h * HEAD, (h + 1) * HEAD), slice((heads + h) * HEAD, (heads + h + 1) * HEAD)
        keys = jnp.concatenate([prior_ref[:, at], own_ref[:, at]], axis=0)
        values = jnp.concatenate([prior_ref[:, of], own_ref[:, of]], axis=0)
        values = jnp.concatenate([values, jnp.ones_like(values)], axis=1)
        for g in range(group // HEAD):
            cols = slice(h * group + g * HEAD, h * group + (g + 1) * HEAD)
            s = lax.dot_general(
                q_ref[slot, :, cols], keys, (((1,), (1,)), ((), ())), preferred_element_type=jnp.float32
            )
            s = jnp.where(allowed, s, -1e30)
            e = jnp.exp2((s - jnp.max(s, axis=-1, keepdims=True)) * (HEAD**-0.5 * math.log2(math.e)))
            o = jnp.dot(e.astype(jnp.bfloat16), values, preferred_element_type=jnp.float32)
            buf[:, cols] = (o[:, :HEAD] / o[:, HEAD:]).astype(jnp.bfloat16)
        part = slice(h * group, (h + 1) * group)
        store = pltpu.make_async_copy(buf.at[:, part], out_ref.at[slot, :, part], sem.at[h])
        store.start()
        stores.append(store)
    for store in stores:
        store.wait()


def attend(slot, lengths, queries, prior, own, so_far):
    count, width = queries.shape[1], queries.shape[2]
    heads = own.shape[1] // (2 * HEAD)
    extra = [] if so_far is None else [so_far]
    return pl.pallas_call(
        functools.partial(attend_kernel, slot),
        in_specs=[vmem()] * 4 + [hbm()] * len(extra),
        out_specs=hbm(),
        out_shape=jax.ShapeDtypeStruct(queries.shape, jnp.bfloat16),
        scratch_shapes=[pltpu.VMEM((count, width), jnp.bfloat16), pltpu.SemaphoreType.DMA((heads,))],
        input_output_aliases={4: 0} if extra else {},
        cost_estimate=cost(8 * count * count * width, 4 << 20),
        compiler_params=pltpu.CompilerParams(vmem_limit_bytes=16 << 20),
        name="attend",
    )(lengths, queries, prior, own, *extra)


def hop(block, axis, count, distance, closed=True):
    return lax.ppermute(block, axis, [(i, (i + distance) % count) for i in range(count) if closed or i + distance < count])


def body(tokens, queries, gains, key_weight, value_weight, lengths):
    key_weight, value_weight = key_weight[0], value_weight[0]
    slots, _, _ = tokens.shape[1:]
    steps = Z // 2 - 1

    rows = {}
    for name, own in (("k", key_weight), ("v", value_weight)):
        rows[name, 0] = own
    for s in range(Z // 2):
        for name in "kv":
            if s < steps or name == "k":
                rows[name, s + 1] = hop(rows[name, s], "z", Z, 1)
            if s < steps or name == "v":
                rows[name, -s - 1] = hop(rows[name, -s], "z", Z, -1)
    rows["v", Z // 2] = rows["v", -(Z // 2)]
    key_rows, value_rows = ([rows[name, c] for c in CAME] for name in "kv")

    acts = []
    for m in range(slots):
        quarters = norm_quarters(m, tokens[0], gains)
        acts.append([quarters[0]] + [hop(quarters[j], "y", Y, j) for j in range(1, Y)])

    held = []
    for m in range(slots):
        near, so_far = 0, None
        if m == 0:
            near = Z - 1
            (so_far,) = products(acts[m], key_rows[:near], value_rows[:near], last=False)
        own, keep, up, down = products(acts[m], key_rows[near:], value_rows[near:], near, so_far)
        up, down = hop(up, "y", Y, 1), hop(down, "y", Y, -1)
        held.append((own, keep, up, down))
    sums = []
    for m in range(slots):
        own, keep, up, down = held[m]
        on_up, on_down = relay(keep, up, down)
        on_up, on_down = hop(on_up, "y", Y, 1), hop(on_down, "y", Y, -1)
        sums.append(totals(own, up, down, on_up, on_down))
    out = None
    for m in range(slots):
        prior = hop(sums[m], ("y", "z"), Y * Z, 1, closed=False)
        out = attend(m, lengths, queries[0], prior, sums[m], out)
    return out[None]


def solution(mesh):
    split = Mesh(mesh.devices.reshape(-1, Y, Z), ("section", "y", "z"))
    spread = ("y", "z")

    return jax.shard_map(
        body,
        mesh=split,
        in_specs=(
            P("section", None, spread, None),
            P("section", None, spread, None),
            P("section", None),
            P("section", spread, None),
            P("section", spread, None),
            P(),
        ),
        out_specs=P("section", None, spread, None),
        check_vma=False,
    )
```
